32 devices in a mesh: dp: 8 (over y, x, core), group: 4 (over z).
Axes of the slice: x: 2, y: 2, z: 4, core: 2. Of those that a mesh axis runs over, the one named last changes fastest.
Arguments:
- tokens: bfloat16 [10240, 768], P(('dp', 'group')), may hold values from -6 to 6
- cotangent: bfloat16 [10240, 768], P(('dp', 'group')), may hold values from -18 to 18
- patch_mask: int32 [10240], P(('dp', 'group')), may hold values 0 or 1
- image_tiles: int32 [32, 3], replicated, may hold values from 0 to 9, as said below
- patches: int32 [32, 3], replicated, may hold values from 0 to 288, as said below
- w_in: bfloat16 [288, 384], replicated, may hold values from -0.375 to 0.375
- b_in: float32 [384], replicated, may hold values from -1 to 1
- w_out: bfloat16 [384, 288], replicated, may hold values from -0.3125 to 0.3125
- ln_gain: float32 [768], replicated, may hold values from 0.5 to 1.5
- ln_shift: float32 [768], replicated, may hold values from -0.5 to 0.5
Outputs:
- dtokens: bfloat16 [10240, 768], P(('dp', 'group'))
- grad_w_in: bfloat16 [288, 384], replicated
- grad_b_in: bfloat16 [384], replicated
- grad_w_out: bfloat16 [384, 288], replicated
- grad_b_out: bfloat16 [288], replicated
- grad_gain: bfloat16 [768], replicated
- grad_shift: bfloat16 [768], replicated
The draws below stay inside these ranges and needn't reach their ends.
Inputs may be any that keep to these rules, and one draw needn't show every extreme that they name: `image_tiles`: entry s of row d is the number of tiles of the s-th image slot of device row d, 0 for an empty slot. A device's tiles sum to at most 10, reached on some device. . An image has at most 9 tiles, reached in every draw. For an image of k tiles, patches lies between max(32, 32 * (k - 1) + 1) and 32 * k; it is 0 for an empty slot.
All inputs are finite; a program needn't handle non-finite values. No bound on the sum of `patch_mask` on one device may be relied on, other than what follows from the above.
Results may differ from the reference program's by a relative error of at most 0.0085.
Values may be sent and summed in bfloat16 or wider, within the bound.
No kernel may reach another device: no remote copies, remote signals or barrier semaphores. Data moves between devices by JAX's collectives and lax.ppermute only.
A program may use at most 64 MiB of HBM per device.

```python
import math
import jax
import jax.numpy as jnp
from jax import lax

C = 768
H = 384
PMAX = 288
TILE = 32
TILES_DEV = 10
IMG_DEV = 3
TOK_DEV = 320
TOKENS = 10240
N_GROUP = 4
DEVICES = 32


def packing_tables(key):
    key = jax.random.fold_in(key, 4242)
    subkeys = jax.random.split(key, 6)
    groups = DEVICES // N_GROUP
    pair_count = N_GROUP // 2
    max_tiles = PMAX // TILE
    first_load = jax.random.randint(subkeys[0], (groups, pair_count), 0, TILES_DEV + 1)
    second_load = jax.random.randint(subkeys[1], (groups, pair_count), 0, TILES_DEV - first_load + 1)
    forced = jax.random.randint(subkeys[2], (), 0, groups)
    chosen_group = jnp.arange(groups)[:, None] == forced
    first_load = jnp.where(chosen_group & (jnp.arange(pair_count)[None, :] == 0), TILES_DEV, first_load)
    second_load = jnp.where(chosen_group, TILES_DEV - first_load, second_load)
    loads = jnp.stack([first_load, second_load], axis=2).reshape(groups, N_GROUP)
    scores = jax.random.randint(subkeys[3], (groups, N_GROUP), 0, 1 << 20) * N_GROUP + jnp.arange(N_GROUP)[None, :]
    shuffle = jnp.argsort(scores, axis=1)
    loads = jnp.take_along_axis(loads, shuffle, axis=1).reshape(DEVICES)
    full_device = loads == TILES_DEV
    remain = loads
    columns = []
    for slot_index in range(IMG_DEV):
        slots_left = IMG_DEV - 1 - slot_index
        low_bound = jnp.maximum(0, remain - max_tiles * slots_left)
        high_bound = jnp.minimum(max_tiles, remain)
        if slot_index == 0:
            low_bound = jnp.where(full_device, high_bound, low_bound)
        taken_tiles = jax.random.randint(jax.random.fold_in(subkeys[4], slot_index), (DEVICES,), low_bound, high_bound + 1)
        columns.append(taken_tiles)
        remain = remain - taken_tiles
    tile_table = jnp.stack(columns, axis=1).astype(jnp.int32)
    filled = tile_table > 0
    low_patch = jnp.where(filled, jnp.maximum(TILE, TILE * (tile_table - 1) + 1), 0)
    high_patch = jnp.where(filled, TILE * tile_table + 1, 1)
    counts = jax.random.randint(subkeys[5], tile_table.shape, low_patch, high_patch)
    return (tile_table, counts.astype(jnp.int32))


def draw_image_tiles(key, part):
    return packing_tables(key)[0]


def draw_patches(key, part):
    return packing_tables(key)[1]


def draw_cotangent(key, part):
    subkeys = jax.random.split(jax.random.fold_in(key, 11), 2)
    base = jnp.clip(jax.random.normal(subkeys[0], (TOKENS, C), jnp.float32), -4.0, 4.0)
    row_scale = jnp.exp(jax.random.uniform(subkeys[1], (TOKENS, 1), jnp.float32, math.log(0.3), math.log(3.0)))
    values = base * row_scale
    return values.astype(jnp.bfloat16)


def touch_ends(drawn, stream_key, smallest, top_value):
    dims = drawn.shape
    index_at = [jax.random.randint(jax.random.fold_in(stream_key, axis), (), 0, dims[axis]) for axis in range(len(dims))]
    drawn = drawn.at[tuple(index_at)].set(smallest)
    longest = dims.index(max(dims))
    index_at[longest] = (index_at[longest] + 1) % dims[longest]
    return drawn.at[tuple(index_at)].set(top_value)


def shard_levels(stream_key, shape, cuts, least, high):
    factor_of, own = 1.0, jax.random.fold_in(stream_key, 6)
    for axis_at, parts in cuts:
        draws = jnp.exp(jax.random.uniform(jax.random.fold_in(own, axis_at), (parts,), jnp.float32, least / len(cuts), high / len(cuts)))
        factor_of = factor_of * jnp.repeat(draws, shape[axis_at] // parts).reshape([-1 if axis == axis_at else 1 for axis in range(len(shape))])
    return factor_of


def scatter_about(rng, dims, scale, bound, shards=(), kind=jnp.bfloat16):
    loudness = shard_levels(rng, dims, shards, -0.22, 0.18) if shards else 1.0
    result = jax.random.normal(rng, dims, jnp.float32) * scale * loudness
    return jnp.minimum(jnp.maximum(result, -bound), bound).astype(kind)


def setup_inputs(seed: int = 0) -> dict:
    arg_keys = jax.random.split(jax.random.key(seed), 11)
    return {
        "tokens": scatter_about(arg_keys[0], (TOKENS, C), 1.0, 6.0, ((0, 32),)),
        "cotangent": draw_cotangent(jax.random.fold_in(arg_keys[10], 71), 0),
        "patch_mask": touch_ends((jax.random.randint(arg_keys[2], (TOKENS,), 0, 8) < 7).astype(jnp.int32), jax.random.fold_in(arg_keys[2], 1), 0, 1),
        "image_tiles": draw_image_tiles(jax.random.fold_in(arg_keys[10], 71), 0),
        "patches": draw_patches(jax.random.fold_in(arg_keys[10], 71), 0),
        "w_in": scatter_about(arg_keys[5], (PMAX, H), PMAX ** -0.5, 0.375),
        "b_in": jnp.clip(jax.random.uniform(arg_keys[6], (H,), jnp.float32, -1.0, 1.0), -1.0, 1.0),
        "w_out": scatter_about(arg_keys[7], (H, PMAX), H ** -0.5, 0.3125),
        "ln_gain": jnp.clip(1.0 + 0.1 * jax.random.normal(arg_keys[8], (C,), jnp.float32), 0.5, 1.5),
        "ln_shift": jnp.clip(jax.random.uniform(arg_keys[9], (C,), jnp.float32, -0.5, 0.5), -0.5, 0.5),
    }


highest = lax.Precision.HIGHEST
ln_epsilon = 1e-05
clip_share = 0.5

def gelu_pair(preact):
    normal_cdf = 0.5 * (1.0 + lax.erf(preact * 0.7071067811865476))
    density = jnp.exp(-0.5 * preact * preact) * 0.3989422804014327
    return (preact * normal_cdf, normal_cdf + preact * density)

def layout(tile_row, patch_row):
    starts = (jnp.cumsum(tile_row) - tile_row).astype(jnp.int32)
    places = jnp.arange(TILES_DEV, dtype=jnp.int32)
    inside = (places[:, None] >= starts[None, :]) & (places[:, None] < (starts + tile_row)[None, :])
    offset = places[:, None] - starts[None, :]
    row_place = offset[:, :, None] * TILE + jnp.arange(TILE, dtype=jnp.int32)[None, None, :]
    alive = lax.optimization_barrier(jnp.sum((inside[:, :, None] & (row_place < patch_row[None, :, None])).astype(jnp.int32), axis=1))
    return (inside, offset, alive)

def device_terms(tok_block, cot_block, mask_block, tile_row, patch_row, w_in, b_in, w_out, ln_gain, ln_shift):
    spans = PMAX // TILE
    inside, offset, alive = layout(tile_row, patch_row)
    alive_rows = (alive.reshape(-1) * mask_block).astype(jnp.float32)
    values = tok_block.astype(jnp.float32)
    center = values - lax.optimization_barrier(jnp.mean(values, axis=1, keepdims=True))
    inv_std = lax.rsqrt(lax.optimization_barrier(jnp.mean(center * center, axis=1, keepdims=True)) + ln_epsilon)
    normal_x = center * inv_std
    normed = ((normal_x * ln_gain + ln_shift) * alive_rows[:, None]).astype(jnp.bfloat16)
    dout = (cot_block.astype(jnp.float32) * alive_rows[:, None]).astype(jnp.bfloat16)
    img_hot = inside.astype(jnp.float32)
    tile_alive = lax.optimization_barrier(jnp.sum(inside.astype(jnp.int32), axis=1))
    span_index = lax.optimization_barrier(jnp.sum(jnp.where(inside, offset, 0), axis=1)).astype(jnp.int32)
    span_hot = ((span_index[:, None] == jnp.arange(spans, dtype=jnp.int32)[None, :]) & (tile_alive[:, None] > 0)).astype(jnp.float32)
    image_index = lax.optimization_barrier(jnp.sum(jnp.where(inside, jnp.arange(IMG_DEV, dtype=jnp.int32)[None, :], 0), axis=1)).astype(jnp.int32)
    alive_tile = tile_alive.astype(jnp.float32)
    rows_in = jnp.take(w_in.reshape(spans, TILE, H).astype(jnp.float32), span_index, axis=0) * alive_tile[:, None, None]
    cols_out = jnp.transpose(jnp.take(w_out.reshape(H, spans, TILE).astype(jnp.float32), span_index, axis=1), (1, 0, 2)) * alive_tile[:, None, None]
    y_tiles = normed.astype(jnp.float32).reshape(TILES_DEV, TILE, C)
    o_tiles = dout.astype(jnp.float32).reshape(TILES_DEV, TILE, C)
    part_pre = jnp.einsum('tpc,tph->tch', y_tiles, rows_in, precision=highest)
    part_dz = jnp.einsum('tpc,thp->tch', o_tiles, cols_out, precision=highest)
    preact = jnp.einsum('ts,tch->sch', img_hot, part_pre, precision=highest) + b_in
    dz_all = jnp.einsum('ts,tch->sch', img_hot, part_dz, precision=highest)
    act, slope = gelu_pair(preact)
    act_b = act.astype(jnp.bfloat16)
    dpre = dz_all * slope
    dpre_b = dpre.astype(jnp.bfloat16)
    grad_b_in = lax.optimization_barrier(jnp.sum(dpre, axis=(0, 1)))
    z_tiles = jnp.take(act_b.astype(jnp.float32), image_index, axis=0)
    da_tiles = jnp.take(dpre_b.astype(jnp.float32), image_index, axis=0)
    grad_in_tiles = jnp.einsum('tpc,tch->tph', y_tiles, da_tiles, precision=highest)
    grad_w_in = jnp.einsum('tj,tph->jph', span_hot, grad_in_tiles, precision=highest).reshape(PMAX, H)
    grad_out_tiles = jnp.einsum('tch,tpc->thp', z_tiles, o_tiles, precision=highest)
    grad_w_out = jnp.einsum('tj,thp->hjp', span_hot, grad_out_tiles, precision=highest).reshape(H, PMAX)
    grad_b_out = jnp.einsum('tj,tp->jp', span_hot, lax.optimization_barrier(jnp.sum(o_tiles, axis=2)), precision=highest).reshape(PMAX)
    dnormed = jnp.einsum('tch,tph->tpc', da_tiles, rows_in, precision=highest).astype(jnp.bfloat16).reshape(TOK_DEV, C)
    d_rows = dnormed.astype(jnp.float32) * alive_rows[:, None]
    grad_gain = lax.optimization_barrier(jnp.sum(d_rows * normal_x, axis=0))
    grad_shift = lax.optimization_barrier(jnp.sum(d_rows, axis=0))
    scaled = d_rows * ln_gain
    inner = lax.optimization_barrier(jnp.mean(scaled * normal_x, axis=1, keepdims=True))
    d_norm = (scaled - lax.optimization_barrier(jnp.mean(scaled, axis=1, keepdims=True)) - normal_x * inner) * inv_std
    dtok = (cot_block.astype(jnp.float32) + d_norm).astype(jnp.bfloat16)
    return ((grad_w_in, grad_b_in, grad_w_out, grad_b_out, grad_gain, grad_shift), dtok)

def reference(tokens, cotangent, patch_mask, image_tiles, patches, w_in, b_in, w_out, ln_gain, ln_shift):
    tok_all = tokens.reshape(DEVICES, TOK_DEV, C)
    cot_all = cotangent.reshape(DEVICES, TOK_DEV, C)
    mask_all = patch_mask.reshape(DEVICES, TOK_DEV)
    start_sums = (jnp.zeros((PMAX, H), jnp.float32), jnp.zeros((H,), jnp.float32), jnp.zeros((H, PMAX), jnp.float32), jnp.zeros((PMAX,), jnp.float32), jnp.zeros((C,), jnp.float32), jnp.zeros((C,), jnp.float32))

    def visit(totals, blocks):
        terms, dtok = device_terms(blocks[0], blocks[1], blocks[2], blocks[3], blocks[4], w_in, b_in, w_out, ln_gain, ln_shift)
        return (tuple((left + right for left, right in zip(totals, terms))), dtok)
    totals, dtoks = lax.scan(visit, start_sums, (tok_all, cot_all, mask_all, image_tiles, patches))
    total = sum((jnp.sum(piece * piece) for piece in totals))
    entries = 2 * PMAX * H + H + PMAX + 2 * C
    factor = jnp.minimum(1.0, clip_share * math.sqrt(entries) / jnp.sqrt(total + 1e-06))
    clipped = tuple(((piece * factor).astype(jnp.bfloat16) for piece in totals))
    return (dtoks.reshape(TOKENS, C), clipped[0], clipped[1], clipped[2], clipped[3], clipped[4], clipped[5])
```

```python
import functools
import math

import jax
import jax.numpy as jnp
from jax import lax
from jax.sharding import PartitionSpec as P

PMAX = 288
TILE = 32


highest = lax.Precision.HIGHEST
ln_epsilon = 1e-05
clip_share = 0.5


def gelu_pair(preact):
    normal_cdf = 0.5 * (1.0 + lax.erf(preact * 0.7071067811865476))
    density = jnp.exp(-0.5 * preact * preact) * 0.3989422804014327
    return (preact * normal_cdf, normal_cdf + preact * density)


def tile_layout(tile_rows, tile_total):
    starts = jnp.cumsum(tile_rows, axis=1) - tile_rows
    places = jnp.arange(tile_total, dtype=jnp.int32)
    inside = (places[None, :, None] >= starts[:, None, :]) & (
        places[None, :, None] < (starts + tile_rows)[:, None, :]
    )
    offset = places[None, :, None] - starts[:, None, :]
    return (inside, offset)


def tile_tables(inside, offset, spans):
    img_hot = inside.astype(jnp.float32)
    tile_alive = jnp.sum(inside.astype(jnp.int32), axis=1)
    span_index = jnp.sum(jnp.where(inside, offset, 0), axis=1)
    span_hot = (
        (span_index[:, None] == jnp.arange(spans, dtype=jnp.int32)[None, :])
        & (tile_alive[:, None] > 0)
    ).astype(jnp.float32)
    image_index = jnp.sum(
        jnp.where(inside, jnp.arange(inside.shape[1], dtype=jnp.int32)[None, :], 0), axis=1
    )
    return (img_hot, span_hot, image_index)


def image_core(normed, dout, inside_tiles, span_hot, w_in, b_in, w_out):
    tile_total, slots = inside_tiles.shape
    spans = span_hot.shape[1]
    hidden = w_in.shape[1]
    tile_len = w_in.shape[0] // spans
    rows, width = normed.shape
    span_bf = span_hot.astype(jnp.bfloat16)
    rows_in = jnp.dot(
        span_bf, w_in.reshape(spans, tile_len * hidden), preferred_element_type=jnp.float32
    )
    rows_in = rows_in.astype(jnp.bfloat16).reshape(rows, hidden)
    cols_out = jnp.einsum(
        "tj,hjp->tph",
        span_bf,
        w_out.reshape(hidden, spans, tile_len),
        preferred_element_type=jnp.float32,
    )
    cols_out = cols_out.astype(jnp.bfloat16).reshape(rows, hidden)
    row_hot = (
        jnp.broadcast_to(inside_tiles[:, None, :], (tile_total, tile_len, slots))
        .reshape(rows, slots)
        .astype(jnp.bfloat16)
    )
    in_wide = (rows_in[:, None, :] * row_hot[:, :, None]).reshape(rows, slots * hidden)
    out_wide = (cols_out[:, None, :] * row_hot[:, :, None]).reshape(rows, slots * hidden)
    preact = (
        jnp.einsum("rc,rk->ck", normed, in_wide, preferred_element_type=jnp.float32).reshape(
            width, slots, hidden
        )
        + b_in
    )
    dz_all = jnp.einsum("rc,rk->ck", dout, out_wide, preferred_element_type=jnp.float32).reshape(
        width, slots, hidden
    )
    act, slope = gelu_pair(preact)
    act_b = act.astype(jnp.bfloat16).reshape(width, slots * hidden)
    dpre = dz_all * slope
    dpre_b = dpre.astype(jnp.bfloat16).reshape(width, slots * hidden)
    grad_b_in = jnp.sum(dpre, axis=(0, 1))
    row_mask = row_hot.astype(jnp.float32)[:, :, None]
    grad_rows_in = jnp.sum(
        jnp.einsum("rc,ck->rk", normed, dpre_b, preferred_element_type=jnp.float32).reshape(
            rows, slots, hidden
        )
        * row_mask,
        axis=1,
    )
    grad_rows_out = jnp.sum(
        jnp.einsum("rc,ck->rk", dout, act_b, preferred_element_type=jnp.float32).reshape(
            rows, slots, hidden
        )
        * row_mask,
        axis=1,
    )
    grad_w_in = jnp.einsum(
        "tj,tph->jph",
        span_hot,
        grad_rows_in.reshape(tile_total, tile_len, hidden),
        precision=highest,
    ).reshape(spans * tile_len, hidden)
    grad_w_out = jnp.einsum(
        "tj,tph->jph",
        span_hot,
        grad_rows_out.reshape(tile_total, tile_len, hidden),
        precision=highest,
    ).reshape(spans * tile_len, hidden)
    out_sums = jnp.sum(dout.astype(jnp.float32), axis=1).reshape(tile_total, tile_len)
    grad_b_out = jnp.einsum("tj,tp->jp", span_hot, out_sums, precision=highest).reshape(-1)
    dnormed = jnp.einsum("rk,ck->rc", in_wide, dpre_b, preferred_element_type=jnp.float32).astype(
        jnp.bfloat16
    )
    return ((grad_w_in, grad_b_in, grad_w_out, grad_b_out), dnormed)


def clip_factor(total, entry_count):
    return jnp.minimum(1.0, clip_share * math.sqrt(entry_count) / jnp.sqrt(total + 1e-06))


AXES = ("dp", "group")
LANES = 128


def swap(x, mask, devices):
    return lax.ppermute(x, AXES, [(i, i ^ mask) for i in range(devices)])


def part(x, index, count):
    size = x.shape[0] // count
    return lax.dynamic_slice_in_dim(x, index * size, size, 0)


def all_sum(flat, dp, group):
    devices = dp * group
    if devices & (devices - 1) or dp < 8:
        return lax.psum(flat, AXES)
    me = lax.axis_index(AXES)
    pair, plane = group, 2 * group
    side = (me // pair) % 2
    spot = (me // plane) % 4
    half = part(flat, side, 2) + swap(
        part(flat, 1 - side, 2).astype(jnp.bfloat16), pair, devices
    ).astype(jnp.float32)
    sent = [swap(part(half, spot ^ k, 4).astype(jnp.bfloat16), k * plane, devices) for k in (1, 2, 3)]
    own = part(half, spot, 4)
    for one in sent:
        own = own + one.astype(jnp.float32)
    own = own.astype(jnp.bfloat16)
    rest = [1 << b for b in range(devices.bit_length() - 1)]
    rest = [m for m in rest if m not in (pair, plane, 2 * plane)]
    while rest:
        if len(rest) > 1:
            low, high = rest[:2]
            rest = rest[2:]
            others = [swap(own, m, devices).astype(jnp.float32) for m in (low, high, low + high)]
            own = (own.astype(jnp.float32) + others[0]) + (others[1] + others[2])
        else:
            own = own.astype(jnp.float32) + swap(own, rest.pop(), devices).astype(jnp.float32)
        own = own.astype(jnp.bfloat16)
    near = [own] + [swap(own, k * plane, devices) for k in (1, 2, 3)]
    stack = jnp.stack(near)
    mine = jnp.concatenate(
        [lax.dynamic_index_in_dim(stack, spot ^ j, 0, keepdims=False) for j in range(4)]
    )
    other = swap(mine, pair, devices)
    return jnp.concatenate(
        [jnp.where(side == 0, mine, other), jnp.where(side == 0, other, mine)]
    ).astype(jnp.float32)


def pad_to(x, size):
    return jnp.pad(x, (0, size - x.shape[0]))


def all_sum_pieces(pieces, dp, group):
    flats = [piece.reshape(-1) for piece in pieces]
    widths = [-(-flat.shape[0] // LANES) * LANES for flat in flats]
    flat = jnp.concatenate([pad_to(flat, width) for flat, width in zip(flats, widths)])
    unit = LANES * 16 * 8
    flat = pad_to(flat, -(-flat.shape[0] // unit) * unit)
    out = all_sum(flat.reshape(-1, LANES), dp, group).reshape(-1)
    results, at = [], 0
    for piece, width in zip(pieces, widths):
        results.append(out[at : at + piece.size].reshape(piece.shape))
        at += width
    return results


def local(
    dp, group, tokens, cotangent, patch_mask, image_tiles, patches, w_in, b_in, w_out, ln_gain, ln_shift
):
    tile_len = TILE
    spans = PMAX // TILE
    tile_total = tokens.shape[0] // tile_len
    me_index = lax.axis_index(("dp", "group"))
    own_tiles = lax.dynamic_slice_in_dim(image_tiles, me_index, 1, 0)
    own_patches = lax.dynamic_slice_in_dim(patches, me_index, 1, 0)
    inside, offset = tile_layout(own_tiles, tile_total)
    row_place = offset[..., None] * tile_len + jnp.arange(tile_len, dtype=jnp.int32)
    alive = jnp.sum(
        (inside[..., None] & (row_place < own_patches[:, None, :, None])).astype(jnp.int32), axis=2
    ).reshape(-1)
    alive_rows = (alive * patch_mask).astype(jnp.float32)
    values = tokens.astype(jnp.float32)
    center = values - jnp.mean(values, axis=1, keepdims=True)
    inv_std = lax.rsqrt(jnp.mean(center * center, axis=1, keepdims=True) + ln_epsilon)
    normal_x = center * inv_std
    normed = ((normal_x * ln_gain + ln_shift) * alive_rows[:, None]).astype(jnp.bfloat16)
    dout = (cotangent.astype(jnp.float32) * alive_rows[:, None]).astype(jnp.bfloat16)
    img_hot, span_hot, image_index = tile_tables(inside[0], offset[0], spans)
    terms, dnormed = image_core(normed, dout, inside[0], span_hot, w_in, b_in, w_out)
    d_rows = dnormed.astype(jnp.float32) * alive_rows[:, None]
    grad_gain = jnp.sum(d_rows * normal_x, axis=0)
    grad_shift = jnp.sum(d_rows, axis=0)
    scaled = d_rows * ln_gain
    inner = jnp.mean(scaled * normal_x, axis=1, keepdims=True)
    d_norm = (scaled - jnp.mean(scaled, axis=1, keepdims=True) - normal_x * inner) * inv_std
    dtokens = (cotangent.astype(jnp.float32) + d_norm).astype(jnp.bfloat16)
    grad_w_in, grad_b_in, grad_w_out, grad_b_out = terms
    pieces = (grad_w_in, grad_b_in, grad_w_out, grad_b_out, grad_gain, grad_shift)
    entry_count = sum((piece.size for piece in pieces))
    summed = all_sum_pieces(pieces, dp, group)
    total = sum((jnp.sum(piece * piece) for piece in summed))
    factor = clip_factor(total, entry_count)
    results = [(piece * factor).astype(jnp.bfloat16) for piece in summed]
    return (dtokens, results[0], results[1], results[2].T, results[3], results[4], results[5])


def solution(mesh):
    return jax.shard_map(
        functools.partial(local, mesh.shape["dp"], mesh.shape["group"]),
        mesh=mesh,
        in_specs=(
            P(("dp", "group"), None),
            P(("dp", "group"), None),
            P(("dp", "group")),
            P(),
            P(),
            P(),
            P(),
            P(),
            P(),
            P(),
        ),
        out_specs=(P(("dp", "group"), None), P(), P(), P(), P(), P(), P()),
        check_vma=False,
    )
```

```python
import functools
import math

import jax
import jax.numpy as jnp
from jax import lax
from jax.experimental import pallas as pl
from jax.experimental.pallas import tpu as pltpu
from jax.sharding import PartitionSpec as P

TILE = 32
LANES = 128
AXES = ("dp", "group")
ln_epsilon = 1e-05
clip_share = 0.5
f32 = jnp.float32
bf16 = jnp.bfloat16
NN = (((1,), (0,)), ((), ()))
NT = (((1,), (1,)), ((), ()))


def dot(left, right, dims=NN):
    return lax.dot_general(left, right, dims, preferred_element_type=f32)


def as_column(row):
    return jnp.transpose(jnp.broadcast_to(row, (LANES, row.shape[1])))


def lane_blocks(x):
    return [x[:, at : at + LANES] for at in range(0, x.shape[1], LANES)]


def fold_lanes(x):
    return functools.reduce(jnp.add, lane_blocks(x))


def row_total(x):
    return jnp.sum(fold_lanes(x), axis=1, keepdims=True)


def half_rows(places, hidden, width):
    used = (hidden // LANES) * places + hidden // LANES + width // LANES
    return -(-used // 64) * 64


def grad_kernel(
    pair,
    me_ref,
    tiles_ref,
    patches_ref,
    tok_ref,
    cot_ref,
    mask_ref,
    w_in_ref,
    b_in_ref,
    w_out_ref,
    gain_ref,
    shift_ref,
    dtok_ref,
    keep_ref,
    send_ref,
    flat_ref,
    y_s,
    o_s,
    dn_s,
    w_in_t,
    w_out_s,
    bias_s,
    alive_s,
    mean_s,
    inv_s,
    gin_s,
    gout_s,
    bin_s,
    bout_s,
):
    rows, width = tok_ref.shape
    places, hidden = w_in_ref.shape
    slots = tiles_ref.shape[0]
    me = me_ref[0]
    tiles = [tiles_ref[s, me] for s in range(slots)]
    counts = [patches_ref[s, me] for s in range(slots)]
    firsts = [sum(tiles[:s], jnp.int32(0)) * TILE for s in range(slots)]
    half = keep_ref.shape[0]
    side = (me // pair) % 2
    gain = gain_ref[...].reshape(1, width)
    shift = shift_ref[...].reshape(1, width)

    w_in_t[...] = jnp.transpose(w_in_ref[...])
    w_out_s[...] = jnp.transpose(w_out_ref[...])
    bias_s[...] = as_column(b_in_ref[...].reshape(1, hidden))
    gin_s[...] = jnp.zeros(gin_s.shape, f32)
    gout_s[...] = jnp.zeros(gout_s.shape, f32)
    bin_s[...] = jnp.zeros(bin_s.shape, f32)
    bout_s[...] = jnp.zeros(bout_s.shape, f32)

    mask_row = mask_ref[...].astype(f32).reshape(1, rows)
    short = -rows % LANES
    kept = as_column(jnp.concatenate([mask_row, jnp.zeros((1, short), f32)], axis=1))[:rows]
    row = lax.broadcasted_iota(jnp.int32, (rows, LANES), 0)
    inside = functools.reduce(
        jnp.logical_or,
        [(row >= first) & (row < first + count) for first, count in zip(firsts, counts)],
    )
    alive_s[...] = jnp.where(inside, kept, 0.0)

    step = 64
    for at in range(0, rows, step):
        piece = slice(at, at + step)
        values = tok_ref[piece, :].astype(f32)
        mean = row_total(values) * (1.0 / width)
        center = values - mean
        inv_std = lax.rsqrt(row_total(center * center) * (1.0 / width) + ln_epsilon)
        mean_s[piece, :] = jnp.broadcast_to(mean, (step, LANES))
        inv_s[piece, :] = jnp.broadcast_to(inv_std, (step, LANES))
        alive = alive_s[piece, :1]
        y_s[piece, :] = ((center * inv_std * gain + shift) * alive).astype(bf16)
        o_s[piece, :] = (cot_ref[piece, :].astype(f32) * alive).astype(bf16)
    tail = slice(rows, y_s.shape[0])
    y_s[tail, :] = jnp.zeros((places, width), bf16)
    o_s[tail, :] = jnp.zeros((places, width), bf16)

    chunk = 256
    third = places // 3

    def image(first, count, window):
        first = pl.multiple_of(first, TILE)
        limit = count * TILE
        lane = lax.broadcasted_iota(jnp.int32, (hidden, window), 1)
        own_in = jnp.where(lane < limit, w_in_t[:, :window].astype(f32), 0.0).astype(bf16)
        own_out = jnp.where(lane < limit, w_out_s[:, :window].astype(f32), 0.0).astype(bf16)
        bias = jnp.concatenate([bias_s[...]] * (chunk // LANES), axis=1)
        gin = jnp.zeros((window, hidden), f32)
        gout = jnp.zeros((window, hidden), f32)
        bin_sum = jnp.zeros((hidden, LANES), f32)
        bout_sum = jnp.zeros((window, LANES), f32)
        for at in range(0, width, chunk):
            cols = slice(at, at + chunk)
            y = y_s[pl.ds(first, window), cols]
            o = o_s[pl.ds(first, window), cols]
            preact = dot(own_in, y) + bias
            dz = dot(own_out, o)
            normal_cdf = 0.5 + 0.5 * lax.erf(preact * 0.7071067811865476)
            density = jnp.exp(-0.5 * preact * preact) * 0.3989422804014327
            act = (preact * normal_cdf).astype(bf16)
            dpre = dz * (normal_cdf + preact * density)
            dpre_b = dpre.astype(bf16)
            bin_sum += fold_lanes(dpre)
            bout_sum += fold_lanes(o.astype(f32))
            gin += dot(y, dpre_b, NT)
            gout += dot(o, act, NT)
            dn_s[pl.ds(first, window), cols] = dot(w_in_ref[:window, :], dpre_b).astype(bf16)
        place = lax.broadcasted_iota(jnp.int32, (window, LANES), 0)
        own = place < limit
        wide = lax.broadcasted_iota(jnp.int32, (window, hidden), 0) < limit
        gin_s[:window, :] += jnp.where(wide, gin, 0.0)
        gout_s[:window, :] += jnp.where(wide, gout, 0.0)
        bin_s[...] += bin_sum
        bout_s[:window, :] += jnp.where(own, bout_sum, 0.0)

    for first, count in zip(firsts, tiles):
        for size in (1, 2, 3):
            low, high = (size - 1) * third // TILE, size * third // TILE

            @pl.when((count > low) & (count <= high))
            def _():
                image(first, count, size * third)

    gain_sum = jnp.zeros((8, width), f32)
    shift_sum = jnp.zeros((8, width), f32)
    for at in range(0, rows, step):
        piece = slice(at, at + step)
        alive = alive_s[piece, :1]
        inv_std = inv_s[piece, :1]
        normal_x = (tok_ref[piece, :].astype(f32) - mean_s[piece, :1]) * inv_std
        d_rows = jnp.where(alive > 0.0, dn_s[piece, :].astype(f32), 0.0)
        scaled_x = d_rows * normal_x
        gain_sum += jnp.sum(scaled_x.reshape(step // 8, 8, width), axis=0)
        shift_sum += jnp.sum(d_rows.reshape(step // 8, 8, width), axis=0)
        scaled = d_rows * gain
        middle = row_total(scaled) * (1.0 / width)
        inner = row_total(scaled_x * gain) * (1.0 / width)
        d_norm = (scaled - middle - normal_x * inner) * inv_std
        dtok_ref[piece, :] = (cot_ref[piece, :].astype(f32) + d_norm).astype(bf16)

    blocks = hidden // LANES
    small = blocks * places
    pairs = (
        (gin_s, bin_s[...], gain_sum),
        (gout_s, bout_s[...], shift_sum),
    )
    for which, (weights, bias_part, wide_part) in enumerate(pairs):
        base = which * half
        for j in range(blocks):
            flat_ref[base + j * places : base + (j + 1) * places, :] = weights[
                :, j * LANES : (j + 1) * LANES
            ]
        flat_ref[base + small : base + half, :] = jnp.zeros((half - small, LANES), f32)
        bias_row = jnp.sum(jnp.transpose(bias_part), axis=0, keepdims=True)
        wide_row = jnp.sum(wide_part, axis=0, keepdims=True)
        at = base + small
        for block in lane_blocks(bias_row) + lane_blocks(wide_row):
            flat_ref[at : at + 1, :] = block
            at += 1
    keep_ref[...] = flat_ref[pl.ds(pl.multiple_of(side * half, 16), half), :]
    send_ref[...] = flat_ref[pl.ds(pl.multiple_of((1 - side) * half, 16), half), :].astype(bf16)


def all_terms(pair, me, tokens, cotangent, mask, image_tiles, patches, w_in, b_in, w_out, gain, shift):
    rows, width = tokens.shape
    places, hidden = w_in.shape
    half = half_rows(places, hidden, width)
    smem = pl.BlockSpec(memory_space=pltpu.SMEM)
    vmem = pl.BlockSpec(memory_space=pltpu.VMEM)
    return pl.pallas_call(
        functools.partial(grad_kernel, pair),
        name="terms",
        out_shape=(
            jax.ShapeDtypeStruct((rows, width), bf16),
            pltpu.VMEM((half, LANES), f32),
            pltpu.VMEM((half, LANES), bf16),
        ),
        in_specs=[smem] * 3 + [vmem] * 8,
        out_specs=(vmem, vmem, vmem),
        scratch_shapes=[
            pltpu.VMEM((2 * half, LANES), f32),
            pltpu.VMEM((rows + places, width), bf16),
            pltpu.VMEM((rows + places, width), bf16),
            pltpu.VMEM((rows + places, width), bf16),
            pltpu.VMEM((hidden, places), bf16),
            pltpu.VMEM((hidden, places), bf16),
            pltpu.VMEM((hidden, LANES), f32),
            pltpu.VMEM((rows, LANES), f32),
            pltpu.VMEM((rows, LANES), f32),
            pltpu.VMEM((rows, LANES), f32),
            pltpu.VMEM((places, hidden), f32),
            pltpu.VMEM((places, hidden), f32),
            pltpu.VMEM((hidden, LANES), f32),
            pltpu.VMEM((hidden, LANES), f32),
        ],
    )(
        me.reshape(1),
        image_tiles.T,
        patches.T,
        tokens,
        cotangent,
        mask,
        w_in,
        b_in,
        w_out.T,
        gain,
        shift,
    )


def swap(x, mask, devices):
    return lax.ppermute(x, AXES, [(i, i ^ mask) for i in range(devices)])


def part(x, index, count):
    size = x.shape[0] // count
    return lax.dynamic_slice_in_dim(x, index * size, size, 0)


def all_sum(keep, send, dp, group):
    devices = dp * group
    me = lax.axis_index(AXES)
    pair, plane = group, 2 * group
    spot = (me // plane) % 4
    if devices & (devices - 1) or dp < 8:
        raise NotImplementedError("device count")
    half = keep + swap(send, pair, devices).astype(f32)
    sent = [swap(part(half, spot ^ k, 4).astype(bf16), k * plane, devices) for k in (1, 2, 3)]
    own = part(half, spot, 4)
    for one in sent:
        own = own + one.astype(f32)
    own = own.astype(bf16)
    rest = [1 << b for b in range(devices.bit_length() - 1)]
    rest = [m for m in rest if m not in (pair, plane, 2 * plane)]
    while rest:
        if len(rest) > 1:
            low, high = rest[:2]
            rest = rest[2:]
            others = [swap(own, m, devices).astype(f32) for m in (low, high, low + high)]
            own = (own.astype(f32) + others[0]) + (others[1] + others[2])
        else:
            own = own.astype(f32) + swap(own, rest.pop(), devices).astype(f32)
        own = own.astype(bf16)
    near = [own] + [swap(own, k * plane, devices) for k in (1, 2, 3)]
    return near, swap(jnp.concatenate(near), pair, devices)


def clip_kernel(
    pair,
    me_ref,
    near0,
    near1,
    near2,
    near3,
    far_ref,
    w_in_ref,
    b_in_ref,
    w_out_ref,
    b_out_ref,
    gain_ref,
    shift_ref,
    sum_s,
):
    places, hidden = w_in_ref.shape
    width = gain_ref.shape[0]
    size = near0.shape[0]
    half = 4 * size
    me = me_ref[0]
    side = (me // pair) % 2
    spot = (me // (2 * pair)) % 4
    total = jnp.zeros((8, LANES), f32)
    for k, near in enumerate((near0, near1, near2, near3)):
        spread = (spot ^ k) * size
        mine = near[...].astype(f32)
        other = far_ref[k * size : (k + 1) * size, :].astype(f32)
        sum_s[pl.ds(pl.multiple_of(side * half + spread, 16), size), :] = mine
        sum_s[pl.ds(pl.multiple_of((1 - side) * half + spread, 16), size), :] = other
        squares = mine * mine + other * other
        total += jnp.sum(squares.reshape(size // 8, 8, LANES), axis=0)
    total = jnp.sum(total)
    entries = 2 * places * hidden + hidden + places + 2 * width
    total = jnp.full((1, LANES), total, f32)
    factor = jnp.minimum(1.0, clip_share * math.sqrt(entries) * lax.rsqrt(total + 1e-06))
    blocks = hidden // LANES
    small = blocks * places
    for j in range(blocks):
        lanes = slice(j * LANES, (j + 1) * LANES)
        at = j * places
        w_in_ref[:, lanes] = (sum_s[at : at + places, :] * factor).astype(bf16)
        w_out_ref[:, lanes] = (sum_s[half + at : half + at + places, :] * factor).astype(bf16)
    for base, bias_ref, wide_ref in ((0, b_in_ref, gain_ref), (half, b_out_ref, shift_ref)):
        at = base + small
        row = jnp.concatenate([sum_s[at + j : at + j + 1, :] for j in range(blocks)], axis=1)
        size = bias_ref.shape[0]
        bias_ref[...] = (row * factor[:, :1])[:, :size].astype(bf16).reshape(size)
        at += blocks
        row = jnp.concatenate(
            [sum_s[at + j : at + j + 1, :] for j in range(width // LANES)], axis=1
        )
        wide_ref[...] = (row * factor[:, :1]).astype(bf16).reshape(width)


def clipped(pair, me, near, far, places, hidden, width):
    smem = pl.BlockSpec(memory_space=pltpu.SMEM)
    vmem = pl.BlockSpec(memory_space=pltpu.VMEM)
    shapes = [(places, hidden), (hidden,), (places, hidden), (places,), (width,), (width,)]
    outs = pl.pallas_call(
        functools.partial(clip_kernel, pair),
        name="clip",
        out_shape=tuple(jax.ShapeDtypeStruct(shape, bf16) for shape in shapes),
        in_specs=[smem] + [vmem] * 5,
        out_specs=(vmem,) * 6,
        scratch_shapes=[pltpu.VMEM((2 * far.shape[0], LANES), f32)],
    )(me.reshape(1), *[pltpu.with_memory_space_constraint(x, pltpu.VMEM) for x in (*near, far)])
    return outs[0], outs[1], outs[2].T, *outs[3:]


def local(
    dp,
    group,
    tokens,
    cotangent,
    patch_mask,
    image_tiles,
    patches,
    w_in,
    b_in,
    w_out,
    ln_gain,
    ln_shift,
):
    me = lax.axis_index(AXES)
    dtokens, keep, send = all_terms(
        group,
        me,
        tokens,
        cotangent,
        patch_mask,
        image_tiles,
        patches,
        w_in,
        b_in,
        w_out,
        ln_gain,
        ln_shift,
    )
    near, far = all_sum(keep, send, dp, group)
    grads = clipped(group, me, near, far, *w_in.shape, tokens.shape[1])
    return (dtokens, *grads)


def solution(mesh):
    return jax.shard_map(
        functools.partial(local, mesh.shape["dp"], mesh.shape["group"]),
        mesh=mesh,
        in_specs=(
            P(AXES, None),
            P(AXES, None),
            P(AXES),
            P(),
            P(),
            P(),
            P(),
            P(),
            P(),
            P(),
        ),
        out_specs=(P(AXES, None), P(), P(), P(), P(), P(), P()),
        check_vma=False,
    )
```

```python
import functools
import math

import jax
import jax.numpy as jnp
from jax import lax
from jax.experimental import pallas as pl
from jax.experimental.pallas import tpu as pltpu
from jax.sharding import PartitionSpec as P


TILE = 32
LANES = 128
VMEM_LIMIT = 24 * 2**20
AXES = ("dp", "group")
ln_epsilon = 1e-05
clip_share = 0.5
f32 = jnp.float32
bf16 = jnp.bfloat16
NN = (((1,), (0,)), ((), ()))
NT = (((1,), (1,)), ((), ()))


def dot(left, right, dims=NN):
    return lax.dot_general(left, right, dims, preferred_element_type=f32)


def as_column(row):
    return jnp.transpose(jnp.broadcast_to(row, (LANES, row.shape[1])))


def lane_blocks(x):
    return [x[:, at : at + LANES] for at in range(0, x.shape[1], LANES)]


def fold_lanes(x):
    return functools.reduce(jnp.add, lane_blocks(x))


def row_total(x):
    return jnp.sum(fold_lanes(x), axis=1, keepdims=True)


def half_rows(places, hidden, width):
    used = (hidden // LANES) * places + hidden // LANES + width // LANES
    return -(-used // 64) * 64


def grad_kernel(
    pair,
    me_ref,
    tiles_hbm,
    patches_hbm,
    tok_hbm,
    cot_hbm,
    mask_hbm,
    w_in_hbm,
    b_in_hbm,
    w_out_hbm,
    gain_hbm,
    shift_hbm,
    keep_ref,
    send_ref,
    dn_s,
    alive_s,
    mean_s,
    inv_s,
    tiles_ref,
    patches_ref,
    tok_ref,
    cot_ref,
    mask_ref,
    w_in_ref,
    b_in_ref,
    w_out_ref,
    gain_ref,
    shift_ref,
    y_s,
    o_s,
    w_in_t,
    w_out_s,
    bias_s,
    gin_s,
    gout_s,
    bin_s,
    bout_s,
    sems,
):
    sources = (tiles_hbm, patches_hbm, mask_hbm, gain_hbm, shift_hbm, b_in_hbm)
    targets = (tiles_ref, patches_ref, mask_ref, gain_ref, shift_ref, b_in_ref)
    copies = [
        pltpu.make_async_copy(source, target, sems.at[i])
        for i, (source, target) in enumerate(zip(sources, targets))
    ]
    fetch_tok = pltpu.make_async_copy(tok_hbm, tok_ref, sems.at[6])
    fetch_cot = pltpu.make_async_copy(cot_hbm, cot_ref, sems.at[7])
    fetch_in = pltpu.make_async_copy(w_in_hbm, w_in_ref, sems.at[8])
    fetch_out = pltpu.make_async_copy(w_out_hbm, w_out_ref, sems.at[9])
    for copy in copies:
        copy.start()
    for copy in (fetch_tok, fetch_cot, fetch_in, fetch_out):
        copy.start()
    gin_s[...] = jnp.zeros(gin_s.shape, f32)
    gout_s[...] = jnp.zeros(gout_s.shape, f32)
    bin_s[...] = jnp.zeros(bin_s.shape, f32)
    bout_s[...] = jnp.zeros(bout_s.shape, f32)
    tail = slice(tok_ref.shape[0], y_s.shape[0])
    y_s[tail, :] = jnp.zeros((w_in_ref.shape[0], tok_ref.shape[1]), bf16)
    o_s[tail, :] = jnp.zeros((w_in_ref.shape[0], tok_ref.shape[1]), bf16)
    for copy in copies:
        copy.wait()
    fetch_tok.wait()
    fetch_cot.wait()
    rows, width = tok_ref.shape
    places, hidden = w_in_ref.shape
    slots = tiles_ref.shape[0]
    me = me_ref[0]
    tiles = [tiles_ref[s, me] for s in range(slots)]
    counts = [patches_ref[s, me] for s in range(slots)]
    firsts = [sum(tiles[:s], jnp.int32(0)) * TILE for s in range(slots)]
    half = keep_ref.shape[0]
    side = (me // pair) % 2
    gain = gain_ref[...].reshape(1, width)
    shift = shift_ref[...].reshape(1, width)

    mask_row = mask_ref[...].astype(f32).reshape(1, rows)
    short = -rows % LANES
    kept = as_column(jnp.concatenate([mask_row, jnp.zeros((1, short), f32)], axis=1))[:rows]
    row = lax.broadcasted_iota(jnp.int32, (rows, LANES), 0)
    inside = functools.reduce(
        jnp.logical_or,
        [(row >= first) & (row < first + count) for first, count in zip(firsts, counts)],
    )
    alive_s[...] = jnp.where(inside, kept, 0.0)

    step = 64
    for at in range(0, rows, step):
        piece = slice(at, at + step)
        values = tok_ref[piece, :].astype(f32)
        mean = row_total(values) * (1.0 / width)
        center = values - mean
        inv_std = lax.rsqrt(row_total(center * center) * (1.0 / width) + ln_epsilon)
        mean_s[piece, :] = jnp.broadcast_to(mean, (step, LANES))
        inv_s[piece, :] = jnp.broadcast_to(inv_std, (step, LANES))
        alive = alive_s[piece, :1]
        y_s[piece, :] = ((center * inv_std * gain + shift) * alive).astype(bf16)
        o_s[piece, :] = (cot_ref[piece, :].astype(f32) * alive).astype(bf16)
    fetch_in.wait()
    fetch_out.wait()
    w_in_t[...] = jnp.transpose(w_in_ref[...])
    w_out_s[...] = jnp.transpose(w_out_ref[...])
    bias_s[...] = as_column(b_in_ref[...].reshape(1, hidden))

    chunk = 256
    third = places // 3

    def image(first, count, window):
        first = pl.multiple_of(first, TILE)
        limit = count * TILE
        lane = lax.broadcasted_iota(jnp.int32, (hidden, window), 1)
        own_in = jnp.where(lane < limit, w_in_t[:, :window].astype(f32), 0.0).astype(bf16)
        own_out = jnp.where(lane < limit, w_out_s[:, :window].astype(f32), 0.0).astype(bf16)
        bias = jnp.concatenate([bias_s[...]] * (chunk // LANES), axis=1)
        gin = jnp.zeros((window, hidden), f32)
        gout = jnp.zeros((window, hidden), f32)
        bin_sum = jnp.zeros((hidden, LANES), f32)
        bout_sum = jnp.zeros((window, LANES), f32)
        for at in range(0, width, chunk):
            cols = slice(at, at + chunk)
            y = y_s[pl.ds(first, window), cols]
            o = o_s[pl.ds(first, window), cols]
            preact = dot(own_in, y) + bias
            dz = dot(own_out, o)
            normal_cdf = 0.5 + 0.5 * lax.erf(preact * 0.7071067811865476)
            density = jnp.exp(-0.5 * preact * preact) * 0.3989422804014327
            act = (preact * normal_cdf).astype(bf16)
            dpre = dz * (normal_cdf + preact * density)
            dpre_b = dpre.astype(bf16)
            bin_sum += fold_lanes(dpre)
            bout_sum += fold_lanes(o.astype(f32))
            gin += dot(y, dpre_b, NT)
            gout += dot(o, act, NT)
            dn_s[pl.ds(first, window), cols] = dot(w_in_ref[:window, :], dpre_b).astype(bf16)
        place = lax.broadcasted_iota(jnp.int32, (window, LANES), 0)
        own = place < limit
        wide = lax.broadcasted_iota(jnp.int32, (window, hidden), 0) < limit
        gin_s[:window, :] += jnp.where(wide, gin, 0.0)
        gout_s[:window, :] += jnp.where(wide, gout, 0.0)
        bin_s[...] += bin_sum
        bout_s[:window, :] += jnp.where(own, bout_sum, 0.0)

    for first, count in zip(firsts, tiles):
        for size in (1, 2, 3):
            low, high = (size - 1) * third // TILE, size * third // TILE

            @pl.when((count > low) & (count <= high))
            def _():
                image(first, count, size * third)

    gain_sum = jnp.zeros((8, width), f32)
    shift_sum = jnp.zeros((8, width), f32)
    for at in range(0, rows, step):
        piece = slice(at, at + step)
        alive = alive_s[piece, :1]
        inv_std = inv_s[piece, :1]
        normal_x = (tok_ref[piece, :].astype(f32) - mean_s[piece, :1]) * inv_std
        d_rows = jnp.where(alive > 0.0, dn_s[piece, :].astype(f32), 0.0)
        scaled_x = d_rows * normal_x
        gain_sum += jnp.sum(scaled_x.reshape(step // 8, 8, width), axis=0)
        shift_sum += jnp.sum(d_rows.reshape(step // 8, 8, width), axis=0)

    blocks = hidden // LANES
    small = blocks * places
    parts = (
        (gin_s, bin_s[...], gain_sum),
        (gout_s, bout_s[...], shift_sum),
    )

    def write(ref, weights, bias_part, wide_part):
        for j in range(blocks):
            ref[j * places : (j + 1) * places, :] = weights[
                :, j * LANES : (j + 1) * LANES
            ].astype(ref.dtype)
        bias_row = jnp.sum(jnp.transpose(bias_part), axis=0, keepdims=True)
        wide_row = jnp.sum(wide_part, axis=0, keepdims=True)
        rest = lane_blocks(bias_row) + lane_blocks(wide_row)
        rest.append(jnp.zeros((half - small - len(rest), LANES), f32))
        ref[small:half, :] = jnp.concatenate(rest, axis=0).astype(ref.dtype)

    for which in (0, 1):

        @pl.when(side == which)
        def _():
            write(keep_ref, *parts[which])
            write(send_ref, *parts[1 - which])


def token_kernel(
    tok_ref, cot_ref, gain_ref, dn_ref, alive_s, mean_s, inv_s, dtok_ref
):
    rows, width = tok_ref.shape
    gain = gain_ref[...].reshape(1, width)
    step = 64
    for at in range(0, rows, step):
        piece = slice(at, at + step)
        alive = alive_s[piece, :1]
        inv_std = inv_s[piece, :1]
        normal_x = (tok_ref[piece, :].astype(f32) - mean_s[piece, :1]) * inv_std
        d_rows = jnp.where(alive > 0.0, dn_ref[piece, :].astype(f32), 0.0)
        scaled = d_rows * gain
        middle = row_total(scaled) * (1.0 / width)
        inner = row_total(scaled * normal_x) * (1.0 / width)
        d_norm = (scaled - middle - normal_x * inner) * inv_std
        dtok_ref[piece, :] = (cot_ref[piece, :].astype(f32) + d_norm).astype(bf16)


def all_terms(pair, me, tokens, cotangent, mask, image_tiles, patches, w_in, b_in, w_out, gain, shift):
    rows, width = tokens.shape
    places, hidden = w_in.shape
    half = half_rows(places, hidden, width)
    smem = pl.BlockSpec(memory_space=pltpu.SMEM)
    vmem = pl.BlockSpec(memory_space=pltpu.VMEM)
    anywhere = pl.BlockSpec(memory_space=pltpu.HBM)
    keep, send, dn, alive, mean, inv_std = pl.pallas_call(
        functools.partial(grad_kernel, pair),
        name="terms",
        out_shape=(
            pltpu.VMEM((half, LANES), f32),
            pltpu.VMEM((half, LANES), bf16),
            pltpu.VMEM((rows + places, width), bf16),
            pltpu.VMEM((rows, LANES), f32),
            pltpu.VMEM((rows, LANES), f32),
            pltpu.VMEM((rows, LANES), f32),
        ),
        in_specs=[smem] + [anywhere] * 10,
        out_specs=(vmem,) * 6,
        scratch_shapes=[
            pltpu.SMEM(image_tiles.shape[::-1], jnp.int32),
            pltpu.SMEM(patches.shape[::-1], jnp.int32),
            pltpu.VMEM((rows, width), bf16),
            pltpu.VMEM((rows, width), bf16),
            pltpu.VMEM((rows,), jnp.int32),
            pltpu.VMEM((places, hidden), bf16),
            pltpu.VMEM((hidden,), f32),
            pltpu.VMEM((places, hidden), bf16),
            pltpu.VMEM((width,), f32),
            pltpu.VMEM((width,), f32),
            pltpu.VMEM((rows + places, width), bf16),
            pltpu.VMEM((rows + places, width), bf16),
            pltpu.VMEM((hidden, places), bf16),
            pltpu.VMEM((hidden, places), bf16),
            pltpu.VMEM((hidden, LANES), f32),
            pltpu.VMEM((places, hidden), f32),
            pltpu.VMEM((places, hidden), f32),
            pltpu.VMEM((hidden, LANES), f32),
            pltpu.VMEM((hidden, LANES), f32),
            pltpu.SemaphoreType.DMA((10,)),
        ],
        compiler_params=pltpu.CompilerParams(vmem_limit_bytes=VMEM_LIMIT),
    )(
        me.reshape(1),
        *[
            pltpu.with_memory_space_constraint(x, pltpu.HBM)
            for x in (
                image_tiles.T,
                patches.T,
                tokens,
                cotangent,
                mask,
                w_in,
                b_in,
                w_out.T,
                gain,
                shift,
            )
        ],
    )
    kept = [pltpu.with_memory_space_constraint(x, pltpu.VMEM) for x in (dn, alive, mean, inv_std)]
    dtokens = pl.pallas_call(
        token_kernel,
        name="rows",
        out_shape=jax.ShapeDtypeStruct((rows, width), bf16),
        in_specs=[vmem] * 7,
        out_specs=vmem,
        compiler_params=pltpu.CompilerParams(vmem_limit_bytes=VMEM_LIMIT),
    )(tokens, cotangent, gain, *kept)
    return dtokens, keep, send


def swap(x, mask, devices):
    return lax.ppermute(x, AXES, [(i, i ^ mask) for i in range(devices)])


def part(x, index, count):
    size = x.shape[0] // count
    return lax.dynamic_slice_in_dim(x, index * size, size, 0)


def all_sum(keep, send, dp, group):
    devices = dp * group
    me = lax.axis_index(AXES)
    pair, plane = group, 2 * group
    spot = (me // plane) % 4
    if devices & (devices - 1) or dp < 8:
        raise NotImplementedError("device count")
    half = keep + swap(send, pair, devices).astype(f32)
    sent = [swap(part(half, spot ^ k, 4).astype(bf16), k * plane, devices) for k in (1, 2, 3)]
    own = part(half, spot, 4)
    for one in sent:
        own = own + one.astype(f32)
    own = own.astype(bf16)
    rest = [1 << b for b in range(devices.bit_length() - 1)]
    rest = [m for m in rest if m not in (pair, plane, 2 * plane)]
    while rest:
        low, high = (rest + [0])[:2]
        rest = rest[2:]
        masks = [low, high, low + high] if high else [low]
        others = [swap(own, m, devices).astype(f32) for m in masks]
        own = own.astype(f32) + others[0]
        if high:
            own = own + (others[1] + others[2])
        own = own.astype(bf16)
    near = [own] + [swap(own, k * plane, devices) for k in (1, 2, 3)]
    return near, swap(jnp.concatenate(near), pair, devices)


def clip_kernel(
    pair,
    me_ref,
    near0,
    near1,
    near2,
    near3,
    far_ref,
    w_in_ref,
    b_in_ref,
    w_out_ref,
    b_out_ref,
    gain_ref,
    shift_ref,
    sum_s,
):
    places, hidden = w_in_ref.shape
    width = gain_ref.shape[0]
    size = near0.shape[0]
    half = 4 * size
    me = me_ref[0]
    side = (me // pair) % 2
    spot = (me // (2 * pair)) % 4
    total = jnp.zeros((8, LANES), f32)
    for k, near in enumerate((near0, near1, near2, near3)):
        spread = (spot ^ k) * size
        mine = near[...].astype(f32)
        other = far_ref[k * size : (k + 1) * size, :].astype(f32)
        sum_s[pl.ds(pl.multiple_of(side * half + spread, 16), size), :] = mine
        sum_s[pl.ds(pl.multiple_of((1 - side) * half + spread, 16), size), :] = other
        squares = mine * mine + other * other
        total += jnp.sum(squares.reshape(size // 8, 8, LANES), axis=0)
    total = jnp.sum(total)
    entries = 2 * places * hidden + hidden + places + 2 * width
    total = jnp.full((1, LANES), total, f32)
    factor = jnp.minimum(1.0, clip_share * math.sqrt(entries) * lax.rsqrt(total + 1e-06))
    blocks = hidden // LANES
    small = blocks * places
    for j in range(blocks):
        lanes = slice(j * LANES, (j + 1) * LANES)
        at = j * places
        w_in_ref[:, lanes] = (sum_s[at : at + places, :] * factor).astype(bf16)
        w_out_ref[:, lanes] = (sum_s[half + at : half + at + places, :] * factor).astype(bf16)
    for base, bias_ref, wide_ref in ((0, b_in_ref, gain_ref), (half, b_out_ref, shift_ref)):
        at = base + small
        row = jnp.concatenate([sum_s[at + j : at + j + 1, :] for j in range(blocks)], axis=1)
        size = bias_ref.shape[0]
        bias_ref[...] = (row * factor[:, :1])[:, :size].astype(bf16).reshape(size)
        at += blocks
        row = jnp.concatenate(
            [sum_s[at + j : at + j + 1, :] for j in range(width // LANES)], axis=1
        )
        wide_ref[...] = (row * factor[:, :1]).astype(bf16).reshape(width)


def clipped(pair, me, near, far, places, hidden, width):
    smem = pl.BlockSpec(memory_space=pltpu.SMEM)
    vmem = pl.BlockSpec(memory_space=pltpu.VMEM)
    shapes = [(places, hidden), (hidden,), (places, hidden), (places,), (width,), (width,)]
    outs = pl.pallas_call(
        functools.partial(clip_kernel, pair),
        name="clip",
        out_shape=tuple(jax.ShapeDtypeStruct(shape, bf16) for shape in shapes),
        in_specs=[smem] + [vmem] * 5,
        out_specs=(vmem,) * 6,
        scratch_shapes=[pltpu.VMEM((2 * far.shape[0], LANES), f32)],
    )(me.reshape(1), *[pltpu.with_memory_space_constraint(x, pltpu.VMEM) for x in (*near, far)])
    return outs[0], outs[1], outs[2].T, *outs[3:]


def local(
    dp,
    group,
    tokens,
    cotangent,
    patch_mask,
    image_tiles,
    patches,
    w_in,
    b_in,
    w_out,
    ln_gain,
    ln_shift,
):
    me = lax.axis_index(AXES)
    dtokens, keep, send = all_terms(
        group,
        me,
        tokens,
        cotangent,
        patch_mask,
        image_tiles,
        patches,
        w_in,
        b_in,
        w_out,
        ln_gain,
        ln_shift,
    )
    near, far = all_sum(keep, send, dp, group)
    grads = clipped(group, me, near, far, *w_in.shape, tokens.shape[1])
    return (dtokens, *grads)


def solution(mesh):
    return jax.shard_map(
        functools.partial(local, mesh.shape["dp"], mesh.shape["group"]),
        mesh=mesh,
        in_specs=(
            P(AXES, None),
            P(AXES, None),
            P(AXES),
            P(),
            P(),
            P(),
            P(),
            P(),
            P(),
            P(),
        ),
        out_specs=(P(AXES, None), P(), P(), P(), P(), P(), P()),
        check_vma=False,
    )
```

```python
import functools
import math

import jax
import jax.numpy as jnp
from jax import lax
from jax.experimental import pallas as pl
from jax.experimental.pallas import tpu as pltpu
from jax.sharding import PartitionSpec as P


TILE = 32
LANES = 128
VMEM_LIMIT = 24 * 2**20
AXES = ("dp", "group")
ln_epsilon = 1e-05
clip_share = 0.5
f32 = jnp.float32
bf16 = jnp.bfloat16
NN = (((1,), (0,)), ((), ()))
NT = (((1,), (1,)), ((), ()))


def dot(left, right, dims=NN):
    return lax.dot_general(left, right, dims, preferred_element_type=f32)


def as_column(row):
    return jnp.transpose(jnp.broadcast_to(row, (LANES, row.shape[1])))


def lane_blocks(x):
    return [x[:, at : at + LANES] for at in range(0, x.shape[1], LANES)]


def fold_lanes(x):
    return functools.reduce(jnp.add, lane_blocks(x))


def row_total(x):
    return jnp.sum(fold_lanes(x), axis=1, keepdims=True)


def half_rows(places, hidden, width):
    used = (hidden // LANES) * places + hidden // LANES + width // LANES
    return -(-used // 64) * 64


def grad_kernel(
    pair,
    me_ref,
    tiles_hbm,
    patches_hbm,
    tok_hbm,
    cot_hbm,
    mask_hbm,
    w_in_hbm,
    b_in_hbm,
    w_out_hbm,
    gain_hbm,
    shift_hbm,
    keep_ref,
    send_ref,
    dn_s,
    alive_s,
    mean_s,
    inv_s,
    tiles_ref,
    patches_ref,
    tok_ref,
    cot_ref,
    mask_ref,
    w_in_ref,
    b_in_ref,
    w_out_ref,
    gain_ref,
    shift_ref,
    y_s,
    o_s,
    w_in_t,
    w_out_s,
    bias_s,
    gin_s,
    gout_s,
    bin_s,
    bout_s,
    sems,
):
    sources = (tiles_hbm, patches_hbm, mask_hbm, gain_hbm, shift_hbm, b_in_hbm)
    targets = (tiles_ref, patches_ref, mask_ref, gain_ref, shift_ref, b_in_ref)
    copies = [
        pltpu.make_async_copy(source, target, sems.at[i])
        for i, (source, target) in enumerate(zip(sources, targets))
    ]
    fetch_tok = pltpu.make_async_copy(tok_hbm, tok_ref, sems.at[6])
    fetch_cot = pltpu.make_async_copy(cot_hbm, cot_ref, sems.at[7])
    fetch_in = pltpu.make_async_copy(w_in_hbm, w_in_ref, sems.at[8])
    fetch_out = pltpu.make_async_copy(w_out_hbm, w_out_ref, sems.at[9])
    for copy in copies:
        copy.start()
    for copy in (fetch_tok, fetch_cot, fetch_in, fetch_out):
        copy.start()
    gin_s[...] = jnp.zeros(gin_s.shape, f32)
    gout_s[...] = jnp.zeros(gout_s.shape, f32)
    bin_s[...] = jnp.zeros(bin_s.shape, f32)
    bout_s[...] = jnp.zeros(bout_s.shape, f32)
    tail = slice(tok_ref.shape[0], y_s.shape[0])
    y_s[tail, :] = jnp.zeros((w_in_ref.shape[0], tok_ref.shape[1]), bf16)
    o_s[tail, :] = jnp.zeros((w_in_ref.shape[0], tok_ref.shape[1]), bf16)
    for copy in copies:
        copy.wait()
    fetch_tok.wait()
    fetch_cot.wait()
    rows, width = tok_ref.shape
    places, hidden = w_in_ref.shape
    slots = tiles_ref.shape[0]
    me = me_ref[0]
    tiles = [tiles_ref[s, me] for s in range(slots)]
    counts = [patches_ref[s, me] for s in range(slots)]
    firsts = [sum(tiles[:s], jnp.int32(0)) * TILE for s in range(slots)]
    half = keep_ref.shape[0]
    side = (me // pair) % 2
    gain = gain_ref[...].reshape(1, width)
    shift = shift_ref[...].reshape(1, width)

    mask_row = mask_ref[...].astype(f32).reshape(1, rows)
    short = -rows % LANES
    kept = as_column(jnp.concatenate([mask_row, jnp.zeros((1, short), f32)], axis=1))[:rows]
    row = lax.broadcasted_iota(jnp.int32, (rows, LANES), 0)
    inside = functools.reduce(
        jnp.logical_or,
        [(row >= first) & (row < first + count) for first, count in zip(firsts, counts)],
    )
    alive_s[...] = jnp.where(inside, kept, 0.0)

    step = 64
    for at in range(0, rows, step):
        piece = slice(at, at + step)
        values = tok_ref[piece, :].astype(f32)
        mean = row_total(values) * (1.0 / width)
        center = values - mean
        inv_std = lax.rsqrt(row_total(center * center) * (1.0 / width) + ln_epsilon)
        mean_s[piece, :] = jnp.broadcast_to(mean, (step, LANES))
        inv_s[piece, :] = jnp.broadcast_to(inv_std, (step, LANES))
        alive = alive_s[piece, :1]
        y_s[piece, :] = ((center * inv_std * gain + shift) * alive).astype(bf16)
        o_s[piece, :] = (cot_ref[piece, :].astype(f32) * alive).astype(bf16)
    fetch_in.wait()
    fetch_out.wait()
    w_in_t[...] = jnp.transpose(w_in_ref[...])
    w_out_s[...] = jnp.transpose(w_out_ref[...])
    bias_s[...] = as_column(b_in_ref[...].reshape(1, hidden))

    chunk = width
    third = places // 3

    def image(first, count, window):
        first = pl.multiple_of(first, TILE)
        limit = count * TILE
        lane = lax.broadcasted_iota(jnp.int32, (16, window), 1)
        own_lane = jnp.where(lane < limit, 1.0, 0.0).astype(bf16)
        own_lane = jnp.concatenate([own_lane] * (hidden // 16), axis=0)
        own_in = w_in_t[:, :window] * own_lane
        own_out = w_out_s[:, :window] * own_lane
        bias = jnp.concatenate([bias_s[...]] * (chunk // LANES), axis=1)
        gin = jnp.zeros((window, hidden), f32)
        gout = jnp.zeros((window, hidden), f32)
        bin_sum = jnp.zeros((hidden, LANES), f32)
        bout_sum = jnp.zeros((window, LANES), f32)
        for at in range(0, width, chunk):
            cols = slice(at, at + chunk)
            y = y_s[pl.ds(first, window), cols]
            o = o_s[pl.ds(first, window), cols]
            preact = dot(own_in, y) + bias
            dz = dot(own_out, o)
            normal_cdf = 0.5 + 0.5 * lax.erf(preact * 0.7071067811865476)
            density = jnp.exp(-0.5 * preact * preact) * 0.3989422804014327
            act = (preact * normal_cdf).astype(bf16)
            dpre = dz * (normal_cdf + preact * density)
            dpre_b = dpre.astype(bf16)
            bin_sum += fold_lanes(dpre)
            bout_sum += fold_lanes(o.astype(f32))
            gin += dot(y, dpre_b, NT)
            gout += dot(o, act, NT)
            dn_s[pl.ds(first, window), cols] = dot(w_in_ref[:window, :], dpre_b).astype(bf16)
        place = lax.broadcasted_iota(jnp.int32, (window, LANES), 0)
        own = place < limit
        wide = lax.broadcasted_iota(jnp.int32, (window, hidden), 0) < limit
        gin_s[:window, :] += jnp.where(wide, gin, 0.0)
        gout_s[:window, :] += jnp.where(wide, gout, 0.0)
        bin_s[...] += bin_sum
        bout_s[:window, :] += jnp.where(own, bout_sum, 0.0)

    for first, count in zip(firsts, tiles):
        for size in (1, 2, 3):
            low, high = (size - 1) * third // TILE, size * third // TILE

            @pl.when((count > low) & (count <= high))
            def _():
                image(first, count, size * third)

    gain_sum = jnp.zeros((8, width), f32)
    shift_sum = jnp.zeros((8, width), f32)
    for at in range(0, rows, step):
        piece = slice(at, at + step)
        alive = alive_s[piece, :1]
        inv_std = inv_s[piece, :1]
        normal_x = (tok_ref[piece, :].astype(f32) - mean_s[piece, :1]) * inv_std
        d_rows = jnp.where(alive > 0.0, dn_s[piece, :].astype(f32), 0.0)
        scaled_x = d_rows * normal_x
        gain_sum += jnp.sum(scaled_x.reshape(step // 8, 8, width), axis=0)
        shift_sum += jnp.sum(d_rows.reshape(step // 8, 8, width), axis=0)

    blocks = hidden // LANES
    small = blocks * places
    parts = (
        (gin_s, bin_s[...], gain_sum),
        (gout_s, bout_s[...], shift_sum),
    )

    def write(ref, weights, bias_part, wide_part):
        for j in range(blocks):
            ref[j * places : (j + 1) * places, :] = weights[
                :, j * LANES : (j + 1) * LANES
            ].astype(ref.dtype)
        bias_row = jnp.sum(jnp.transpose(bias_part), axis=0, keepdims=True)
        wide_row = jnp.sum(wide_part, axis=0, keepdims=True)
        rest = lane_blocks(bias_row) + lane_blocks(wide_row)
        rest.append(jnp.zeros((half - small - len(rest), LANES), f32))
        ref[small:half, :] = jnp.concatenate(rest, axis=0).astype(ref.dtype)

    for which in (0, 1):

        @pl.when(side == which)
        def _():
            write(keep_ref, *parts[which])
            write(send_ref, *parts[1 - which])


def token_kernel(
    tok_ref, cot_ref, gain_ref, dn_ref, alive_s, mean_s, inv_s, dtok_ref
):
    rows, width = tok_ref.shape
    gain = gain_ref[...].reshape(1, width)
    step = 64
    for at in range(0, rows, step):
        piece = slice(at, at + step)
        alive = alive_s[piece, :1]
        inv_std = inv_s[piece, :1]
        normal_x = (tok_ref[piece, :].astype(f32) - mean_s[piece, :1]) * inv_std
        d_rows = jnp.where(alive > 0.0, dn_ref[piece, :].astype(f32), 0.0)
        scaled = d_rows * gain
        middle = row_total(scaled) * (1.0 / width)
        inner = row_total(scaled * normal_x) * (1.0 / width)
        d_norm = (scaled - middle - normal_x * inner) * inv_std
        dtok_ref[piece, :] = (cot_ref[piece, :].astype(f32) + d_norm).astype(bf16)


def all_terms(pair, me, tokens, cotangent, mask, image_tiles, patches, w_in, b_in, w_out, gain, shift):
    rows, width = tokens.shape
    places, hidden = w_in.shape
    half = half_rows(places, hidden, width)
    smem = pl.BlockSpec(memory_space=pltpu.SMEM)
    vmem = pl.BlockSpec(memory_space=pltpu.VMEM)
    anywhere = pl.BlockSpec(memory_space=pltpu.HBM)
    keep, send, dn, alive, mean, inv_std = pl.pallas_call(
        functools.partial(grad_kernel, pair),
        name="terms",
        out_shape=(
            pltpu.VMEM((half, LANES), f32),
            pltpu.VMEM((half, LANES), bf16),
            pltpu.VMEM((rows + places, width), bf16),
            pltpu.VMEM((rows, LANES), f32),
            pltpu.VMEM((rows, LANES), f32),
            pltpu.VMEM((rows, LANES), f32),
        ),
        in_specs=[smem] + [anywhere] * 10,
        out_specs=(vmem,) * 6,
        scratch_shapes=[
            pltpu.SMEM(image_tiles.shape[::-1], jnp.int32),
            pltpu.SMEM(patches.shape[::-1], jnp.int32),
            pltpu.VMEM((rows, width), bf16),
            pltpu.VMEM((rows, width), bf16),
            pltpu.VMEM((rows,), jnp.int32),
            pltpu.VMEM((places, hidden), bf16),
            pltpu.VMEM((hidden,), f32),
            pltpu.VMEM((places, hidden), bf16),
            pltpu.VMEM((width,), f32),
            pltpu.VMEM((width,), f32),
            pltpu.VMEM((rows + places, width), bf16),
            pltpu.VMEM((rows + places, width), bf16),
            pltpu.VMEM((hidden, places), bf16),
            pltpu.VMEM((hidden, places), bf16),
            pltpu.VMEM((hidden, LANES), f32),
            pltpu.VMEM((places, hidden), f32),
            pltpu.VMEM((places, hidden), f32),
            pltpu.VMEM((hidden, LANES), f32),
            pltpu.VMEM((hidden, LANES), f32),
            pltpu.SemaphoreType.DMA((10,)),
        ],
        compiler_params=pltpu.CompilerParams(vmem_limit_bytes=VMEM_LIMIT),
    )(
        me.reshape(1),
        *[
            pltpu.with_memory_space_constraint(x, pltpu.HBM)
            for x in (
                image_tiles.T,
                patches.T,
                tokens,
                cotangent,
                mask,
                w_in,
                b_in,
                w_out.T,
                gain,
                shift,
            )
        ],
    )
    kept = [pltpu.with_memory_space_constraint(x, pltpu.VMEM) for x in (dn, alive, mean, inv_std)]
    dtokens = pl.pallas_call(
        token_kernel,
        name="rows",
        out_shape=jax.ShapeDtypeStruct((rows, width), bf16),
        in_specs=[vmem] * 7,
        out_specs=vmem,
        compiler_params=pltpu.CompilerParams(vmem_limit_bytes=VMEM_LIMIT),
    )(tokens, cotangent, gain, *kept)
    return dtokens, keep, send


def swap(x, mask, devices):
    return lax.ppermute(x, AXES, [(i, i ^ mask) for i in range(devices)])


def part(x, index, count):
    size = x.shape[0] // count
    return lax.dynamic_slice_in_dim(x, index * size, size, 0)


def all_sum(keep, send, dp, group):
    devices = dp * group
    me = lax.axis_index(AXES)
    pair, plane = group, 2 * group
    spot = (me // plane) % 4
    if devices & (devices - 1) or dp < 8:
        raise NotImplementedError("device count")
    half = keep + swap(send, pair, devices).astype(f32)
    sent = [swap(part(half, spot ^ k, 4).astype(bf16), k * plane, devices) for k in (1, 2, 3)]
    own = part(half, spot, 4)
    for one in sent:
        own = own + one.astype(f32)
    own = own.astype(bf16)
    rest = [1 << b for b in range(devices.bit_length() - 1)]
    rest = [m for m in rest if m not in (pair, plane, 2 * plane)]
    while rest:
        low, high = (rest + [0])[:2]
        rest = rest[2:]
        masks = [low, high, low + high] if high else [low]
        others = [swap(own, m, devices).astype(f32) for m in masks]
        own = own.astype(f32) + others[0]
        if high:
            own = own + (others[1] + others[2])
        own = own.astype(bf16)
    near = [own] + [swap(own, k * plane, devices) for k in (1, 2, 3)]
    return near, swap(jnp.concatenate(near), pair, devices)


def clip_kernel(
    pair,
    me_ref,
    near0,
    near1,
    near2,
    near3,
    far_ref,
    w_in_ref,
    b_in_ref,
    w_out_ref,
    b_out_ref,
    gain_ref,
    shift_ref,
    sum_s,
):
    places, hidden = w_in_ref.shape
    width = gain_ref.shape[0]
    size = near0.shape[0]
    half = 4 * size
    me = me_ref[0]
    side = (me // pair) % 2
    spot = (me // (2 * pair)) % 4
    total = jnp.zeros((8, LANES), f32)
    for k, near in enumerate((near0, near1, near2, near3)):
        spread = (spot ^ k) * size
        mine = near[...].astype(f32)
        other = far_ref[k * size : (k + 1) * size, :].astype(f32)
        sum_s[pl.ds(pl.multiple_of(side * half + spread, 16), size), :] = mine
        sum_s[pl.ds(pl.multiple_of((1 - side) * half + spread, 16), size), :] = other
        squares = mine * mine + other * other
        total += jnp.sum(squares.reshape(size // 8, 8, LANES), axis=0)
    total = jnp.sum(total)
    entries = 2 * places * hidden + hidden + places + 2 * width
    total = jnp.full((1, LANES), total, f32)
    factor = jnp.minimum(1.0, clip_share * math.sqrt(entries) * lax.rsqrt(total + 1e-06))
    blocks = hidden // LANES
    small = blocks * places
    for j in range(blocks):
        lanes = slice(j * LANES, (j + 1) * LANES)
        at = j * places
        w_in_ref[:, lanes] = (sum_s[at : at + places, :] * factor).astype(bf16)
        w_out_ref[:, lanes] = (sum_s[half + at : half + at + places, :] * factor).astype(bf16)
    for base, bias_ref, wide_ref in ((0, b_in_ref, gain_ref), (half, b_out_ref, shift_ref)):
        at = base + small
        row = jnp.concatenate([sum_s[at + j : at + j + 1, :] for j in range(blocks)], axis=1)
        size = bias_ref.shape[0]
        bias_ref[...] = (row * factor[:, :1])[:, :size].astype(bf16).reshape(size)
        at += blocks
        row = jnp.concatenate(
            [sum_s[at + j : at + j + 1, :] for j in range(width // LANES)], axis=1
        )
        wide_ref[...] = (row * factor[:, :1]).astype(bf16).reshape(width)


def clipped(pair, me, near, far, places, hidden, width):
    smem = pl.BlockSpec(memory_space=pltpu.SMEM)
    vmem = pl.BlockSpec(memory_space=pltpu.VMEM)
    shapes = [(places, hidden), (hidden,), (places, hidden), (places,), (width,), (width,)]
    outs = pl.pallas_call(
        functools.partial(clip_kernel, pair),
        name="clip",
        out_shape=tuple(jax.ShapeDtypeStruct(shape, bf16) for shape in shapes),
        in_specs=[smem] + [vmem] * 5,
        out_specs=(vmem,) * 6,
        scratch_shapes=[pltpu.VMEM((2 * far.shape[0], LANES), f32)],
    )(me.reshape(1), *[pltpu.with_memory_space_constraint(x, pltpu.VMEM) for x in (*near, far)])
    return outs[0], outs[1], outs[2].T, *outs[3:]


def local(
    dp,
    group,
    tokens,
    cotangent,
    patch_mask,
    image_tiles,
    patches,
    w_in,
    b_in,
    w_out,
    ln_gain,
    ln_shift,
):
    me = lax.axis_index(AXES)
    dtokens, keep, send = all_terms(
        group,
        me,
        tokens,
        cotangent,
        patch_mask,
        image_tiles,
        patches,
        w_in,
        b_in,
        w_out,
        ln_gain,
        ln_shift,
    )
    near, far = all_sum(keep, send, dp, group)
    grads = clipped(group, me, near, far, *w_in.shape, tokens.shape[1])
    return (dtokens, *grads)


def solution(mesh):
    return jax.shard_map(
        functools.partial(local, mesh.shape["dp"], mesh.shape["group"]),
        mesh=mesh,
        in_specs=(
            P(AXES, None),
            P(AXES, None),
            P(AXES),
            P(),
            P(),
            P(),
            P(),
            P(),
            P(),
            P(),
        ),
        out_specs=(P(AXES, None), P(), P(), P(), P(), P(), P()),
        check_vma=False,
    )
```
